32 devices in a mesh: fsdp: 32 (over z, y, x, core).
Axes of the slice: x: 2, y: 2, z: 4, core: 2. Of those that a mesh axis runs over, the one named last changes fastest.
Arguments:
- hidden_in: bfloat16 [64, 256, 2048], P('fsdp')
- grad_out: bfloat16 [64, 256, 2048], P('fsdp')
- gain_attn: bfloat16 [1, 2048], replicated
- gain_mlp: bfloat16 [1, 2048], replicated
- w_q: bfloat16 [1, 2048, 32, 64], P(None, 'fsdp')
- w_k: bfloat16 [1, 2048, 4, 64], P(None, 'fsdp')
- w_v: bfloat16 [1, 2048, 4, 64], P(None, 'fsdp')
- w_o: bfloat16 [1, 2048, 2048], P(None, 'fsdp')
- w_gate: bfloat16 [1, 2048, 5632], P(None, 'fsdp')
- w_up: bfloat16 [1, 2048, 5632], P(None, 'fsdp')
- w_down: bfloat16 [1, 5632, 2048], P(None, 'fsdp')
- a_q: float32 [1, 2048, 64], replicated
- b_q: float32 [1, 64, 2048], replicated
- a_k: float32 [1, 2048, 64], replicated
- b_k: float32 [1, 64, 256], replicated
- a_v: float32 [1, 2048, 64], replicated
- b_v: float32 [1, 64, 256], replicated
- a_o: float32 [1, 2048, 64], replicated
- b_o: float32 [1, 64, 2048], replicated
- a_gate: float32 [1, 2048, 64], replicated
- b_gate: float32 [1, 64, 5632], replicated
- a_up: float32 [1, 2048, 64], replicated
- b_up: float32 [1, 64, 5632], replicated
- a_down: float32 [1, 5632, 64], replicated
- b_down: float32 [1, 64, 2048], replicated
Outputs:
- output 1: bfloat16 [64, 256, 2048], P('fsdp')
- output 2: float32 [1, 2048, 64], replicated
- output 3: float32 [1, 64, 2048], replicated
- output 4: float32 [1, 2048, 64], replicated
- output 5: float32 [1, 64, 256], replicated
- output 6: float32 [1, 2048, 64], replicated
- output 7: float32 [1, 64, 256], replicated
- output 8: float32 [1, 2048, 64], replicated
- output 9: float32 [1, 64, 2048], replicated
- output 10: float32 [1, 2048, 64], replicated
- output 11: float32 [1, 64, 5632], replicated
- output 12: float32 [1, 2048, 64], replicated
- output 13: float32 [1, 64, 5632], replicated
- output 14: float32 [1, 5632, 64], replicated
- output 15: float32 [1, 64, 2048], replicated
All inputs are finite; a program needn't handle non-finite values.
Results may differ from the reference program's by a relative error of at most 0.02.
Values are sent between devices in bfloat16 or wider.
A program may use at most 1 GiB of HBM per device.

```python
import math
import jax
import jax.numpy as jnp
from jax import lax

H = 2048
FF = 5632
HEADS = 32
KV_HEADS = 4
HEAD = 64
RANK = 64
LAYERS = 1
SEQ = 256
SEQS_DEV = 2
FSDP = 32
NUM_SEQS = FSDP * SEQS_DEV
QDIM = HEADS * HEAD
KDIM = KV_HEADS * HEAD
BLOCK_SEQS = math.gcd(NUM_SEQS, max(1, 4096 // SEQ))
LORA_SCALE = 2.0
NORM_EPS = 1e-5
ROPE_BASE = 10000.0
LORA_NAMES = ('q', 'k', 'v', 'o', 'gate', 'up', 'down')
LORA_DIMS = ((H, QDIM), (H, KDIM), (H, KDIM), (QDIM, H), (H, FF), (H, FF), (FF, H))


def setup_inputs(seed: int = 0) -> dict:
    rng_keys = jax.random.split(jax.random.key(seed), 26)

    def draw_normal(key_idx, arr_shape, std_scale):
        return jax.random.normal(rng_keys[key_idx], arr_shape, jnp.float32) * std_scale

    inputs = {
        'hidden_in': draw_normal(0, (NUM_SEQS, SEQ, H), 1.0).astype(jnp.bfloat16),
        'grad_out': draw_normal(1, (NUM_SEQS, SEQ, H), (NUM_SEQS * SEQ) ** -0.5).astype(jnp.bfloat16),
        'gain_attn': (1.0 + draw_normal(2, (LAYERS, H), 0.25)).astype(jnp.bfloat16),
        'gain_mlp': (1.0 + draw_normal(3, (LAYERS, H), 0.25)).astype(jnp.bfloat16),
        'w_q': draw_normal(4, (LAYERS, H, HEADS, HEAD), H ** -0.5).astype(jnp.bfloat16),
        'w_k': draw_normal(5, (LAYERS, H, KV_HEADS, HEAD), H ** -0.5).astype(jnp.bfloat16),
        'w_v': draw_normal(6, (LAYERS, H, KV_HEADS, HEAD), H ** -0.5).astype(jnp.bfloat16),
        'w_o': draw_normal(7, (LAYERS, QDIM, H), QDIM ** -0.5).astype(jnp.bfloat16),
        'w_gate': draw_normal(8, (LAYERS, H, FF), H ** -0.5).astype(jnp.bfloat16),
        'w_up': draw_normal(9, (LAYERS, H, FF), H ** -0.5).astype(jnp.bfloat16),
        'w_down': draw_normal(10, (LAYERS, FF, H), FF ** -0.5).astype(jnp.bfloat16),
    }
    for pos_idx in range(7):
        fan_in, fan_out = LORA_DIMS[pos_idx]
        inputs['a_' + LORA_NAMES[pos_idx]] = draw_normal(11 + 2 * pos_idx, (LAYERS, fan_in, RANK), fan_in ** -0.5)
        inputs['b_' + LORA_NAMES[pos_idx]] = draw_normal(12 + 2 * pos_idx, (LAYERS, RANK, fan_out), 0.2 * RANK ** -0.5)
    return inputs


def rms_norm(hidden, gain_vec):
    hid_f32 = hidden.astype(jnp.float32)
    inv_rms = lax.rsqrt(jnp.mean(hid_f32 * hid_f32, axis=-1, keepdims=True) + NORM_EPS)
    return (hid_f32 * inv_rms * gain_vec.astype(jnp.float32)).astype(jnp.bfloat16)


def project(in_acts, weight, a_mat, b_mat):
    base_out = jnp.dot(in_acts, weight, preferred_element_type=jnp.float32)
    lora_mid = jnp.dot(in_acts.astype(jnp.float32), a_mat)
    return base_out + LORA_SCALE * jnp.dot(lora_mid, b_mat)


def apply_rope(rot_in):
    half_dim = HEAD // 2
    inv_freq = ROPE_BASE ** (-jnp.arange(half_dim, dtype=jnp.float32) * 2.0 / HEAD)
    angles = jnp.arange(SEQ, dtype=jnp.float32)[:, None] * inv_freq[None, :]
    cos_t = jnp.cos(angles)[:, None, :]
    sin_t = jnp.sin(angles)[:, None, :]
    first_half = rot_in[..., :half_dim]
    second_half = rot_in[..., half_dim:]
    return jnp.concatenate([first_half * cos_t - second_half * sin_t, second_half * cos_t + first_half * sin_t], axis=-1)


def attend(q_seq, k_seq, v_seq):
    q_rot = apply_rope(q_seq).astype(jnp.bfloat16).reshape(SEQ, KV_HEADS, HEADS // KV_HEADS, HEAD)
    k_rot = apply_rope(k_seq).astype(jnp.bfloat16)
    scores = jnp.einsum('qkgd,skd->kgqs', q_rot.astype(jnp.float32), k_rot.astype(jnp.float32)) * (HEAD ** -0.5)
    causal = jnp.arange(SEQ)[:, None] >= jnp.arange(SEQ)[None, :]
    attn_probs = jax.nn.softmax(jnp.where(causal, scores, -1e30), axis=-1).astype(jnp.bfloat16)
    attn_out = jnp.einsum('kgqs,skd->qkgd', attn_probs.astype(jnp.float32), v_seq.astype(jnp.float32))
    return attn_out.astype(jnp.bfloat16).reshape(SEQ, QDIM)


def layer_fwd(hidden, base_w, lora_w):
    gain_attn, gain_mlp, w_q, w_k, w_v, w_o, w_gate, w_up, w_down = base_w
    a_q, b_q, a_k, b_k, a_v, b_v, a_o, b_o, a_gate, b_gate, a_up, b_up, a_down, b_down = lora_w
    tok_rows = hidden.reshape(-1, H)
    normed = rms_norm(tok_rows, gain_attn)
    q_all = project(normed, w_q.reshape(H, QDIM), a_q, b_q).reshape(-1, SEQ, HEADS, HEAD)
    k_all = project(normed, w_k.reshape(H, KDIM), a_k, b_k).reshape(-1, SEQ, KV_HEADS, HEAD)
    v_all = project(normed, w_v.reshape(H, KDIM), a_v, b_v).astype(jnp.bfloat16).reshape(-1, SEQ, KV_HEADS, HEAD)
    attn_out = lax.map(lambda qkv_seq: attend(qkv_seq[0], qkv_seq[1], qkv_seq[2]), (q_all, k_all, v_all)).reshape(-1, QDIM)
    h_mid = (tok_rows.astype(jnp.float32) + project(attn_out, w_o, a_o, b_o)).astype(jnp.bfloat16)
    normed_mlp = rms_norm(h_mid, gain_mlp)
    gate_pre = project(normed_mlp, w_gate, a_gate, b_gate)
    up_pre = project(normed_mlp, w_up, a_up, b_up)
    mlp_act = (jax.nn.silu(gate_pre) * up_pre).astype(jnp.bfloat16)
    layer_out = (h_mid.astype(jnp.float32) + project(mlp_act, w_down, a_down, b_down)).astype(jnp.bfloat16)
    return layer_out.reshape(hidden.shape)


def reference(hidden_in, grad_out, gain_attn, gain_mlp, w_q, w_k, w_v, w_o, w_gate, w_up, w_down, a_q, b_q, a_k, b_k, a_v, b_v, a_o, b_o, a_gate, b_gate, a_up, b_up, a_down, b_down):
    base_stack = (gain_attn, gain_mlp, w_q, w_k, w_v, w_o, w_gate, w_up, w_down)
    lora_stack = (a_q, b_q, a_k, b_k, a_v, b_v, a_o, b_o, a_gate, b_gate, a_up, b_up, a_down, b_down)

    def fwd_step(carry_h, layer_w):
        return layer_fwd(carry_h, layer_w[0], layer_w[1]), carry_h

    def bwd_step(carry_d, layer_xs):
        base_w, lora_w, layer_in = layer_xs
        pullback = jax.vjp(lambda hid_arg, lora_arg: layer_fwd(hid_arg, base_w, lora_arg), layer_in, lora_w)[1]
        return pullback(carry_d)

    def block_step(grad_acc, block_in):
        hid_block, cot_block = block_in
        final_h, saved_in = lax.scan(fwd_step, hid_block, (base_stack, lora_stack))
        d_lora = lax.scan(bwd_step, cot_block, (base_stack, lora_stack, saved_in), reverse=True)[1]
        return jax.tree.map(lambda total_g, part_g: total_g + part_g, grad_acc, d_lora), final_h

    num_blocks = NUM_SEQS // BLOCK_SEQS
    grad_init = jax.tree.map(jnp.zeros_like, lora_stack)
    block_xs = (hidden_in.reshape(num_blocks, BLOCK_SEQS, SEQ, H), grad_out.reshape(num_blocks, BLOCK_SEQS, SEQ, H))
    grad_acc, h_blocks = lax.scan(block_step, grad_init, block_xs)
    return (h_blocks.reshape(NUM_SEQS, SEQ, H),) + tuple(grad_acc)
```

```python
import functools

import jax
import jax.numpy as jnp
from jax import lax
from jax.experimental import pallas as pl
from jax.experimental.pallas import tpu as pltpu
from jax.sharding import PartitionSpec as P

LORA_SCALE = 2.0
NORM_EPS = 1e-5
ROPE_BASE = 10000.0
AXIS = 'fsdp'
F32 = jnp.float32
BF16 = jnp.bfloat16
FF_CHUNK = 512
ROW_CHUNK = 16


def rms_norm(hidden, gain_vec):
    hid_f32 = hidden.astype(F32)
    inv_rms = lax.rsqrt(jnp.mean(hid_f32 * hid_f32, axis=-1, keepdims=True) + NORM_EPS)
    return (hid_f32 * inv_rms * gain_vec.astype(F32)).astype(BF16)


def apply_rope(rot_in):
    seq_len, head_dim = rot_in.shape[1], rot_in.shape[3]
    half_dim = head_dim // 2
    inv_freq = ROPE_BASE ** (-jnp.arange(half_dim, dtype=F32) * 2.0 / head_dim)
    angles = jnp.arange(seq_len, dtype=F32)[:, None] * inv_freq[None, :]
    cos_t = jnp.cos(angles)[:, None, :]
    sin_t = jnp.sin(angles)[:, None, :]
    first_half = rot_in[..., :half_dim]
    second_half = rot_in[..., half_dim:]
    return jnp.concatenate([first_half * cos_t - second_half * sin_t, second_half * cos_t + first_half * sin_t], axis=-1)


def attn_core(q_proj, k_proj, v_proj):
    n_seq, seq_len, n_heads, head_dim = q_proj.shape
    kv_heads = k_proj.shape[2]
    q_rot = apply_rope(q_proj).astype(BF16).reshape(n_seq, seq_len, kv_heads, n_heads // kv_heads, head_dim)
    k_rot = apply_rope(k_proj).astype(BF16)
    scores = jnp.einsum('bqkgd,bskd->bkgqs', q_rot, k_rot, preferred_element_type=F32) * (head_dim ** -0.5)
    causal = jnp.arange(seq_len)[:, None] >= jnp.arange(seq_len)[None, :]
    attn_probs = jax.nn.softmax(jnp.where(causal, scores, -1e30), axis=-1).astype(BF16)
    attn_out = jnp.einsum('bkgqs,bskd->bqkgd', attn_probs, v_proj, preferred_element_type=F32)
    return attn_out.astype(BF16).reshape(n_seq * seq_len, n_heads * head_dim)


def dot_nn(a, b):
    return lax.dot_general(a, b, (((1,), (0,)), ((), ())), preferred_element_type=F32)


def dot_nt(a, b):
    return lax.dot_general(a, b, (((1,), (1,)), ((), ())), preferred_element_type=F32)


def dot_tn(a, b):
    return lax.dot_general(a, b, (((0,), (0,)), ((), ())), preferred_element_type=F32)


def coords():
    me = lax.axis_index(AXIS)
    core = lax.rem(me, 2)
    x = lax.rem(me // 2, 2)
    y = lax.rem(me // 4, 2)
    z = me // 8
    return me, z, y, x, core


def peers(me, z, y, x, core):
    z_peers = [me + 8 * (lax.rem(z + k, 4) - z) for k in (1, 2, 3)]
    return z_peers, me + 4 * (1 - 2 * y), me + 2 * (1 - 2 * x), me + 1 - 2 * core


def entry_barrier(devices):
    barrier = pltpu.get_barrier_semaphore()
    for dev in devices:
        pl.semaphore_signal(barrier, inc=1, device_id=(dev,), device_id_type=pl.DeviceIdType.MESH)
    pl.semaphore_wait(barrier, len(devices))


def remote(src, dst, send_sem, recv_sem, dev):
    return pltpu.make_async_remote_copy(src_ref=src, dst_ref=dst, send_sem=send_sem, recv_sem=recv_sem,
                                        device_id=(dev,), device_id_type=pl.DeviceIdType.MESH)


def gather_rows_kernel(n_arr, *refs):
    srcs, outs = refs[:n_arr], refs[n_arr:2 * n_arr]
    send, recv, own_sem = refs[2 * n_arr:]
    me, z, y, x, core = coords()
    z_peers, y_peer, x_peer, partner = peers(me, z, y, x, core)
    entry_barrier(z_peers + [y_peer, x_peer, partner])
    n_chunks = srcs[0].shape[0] // ROW_CHUNK
    half = ROW_CHUNK // 2

    def own_copy(i):
        return pltpu.make_async_copy(srcs[i], outs[i].at[z, y, x, core], own_sem.at[i])

    for i in range(n_arr):
        own_copy(i).start()
    for i in range(n_arr):
        own_copy(i).wait()

    def phase_copies(chunk, phase, par, i):
        out = outs[i]
        r0 = chunk * ROW_CHUNK
        all_rows, a_rows, b_rows = pl.ds(r0, ROW_CHUNK), pl.ds(r0, half), pl.ds(r0 + half, half)
        if phase == 0:
            items = [(srcs[i].at[all_rows], out.at[z, y, x, core, all_rows], dev) for dev in z_peers]
        elif phase == 1:
            a, b = out.at[:, y, x, core, a_rows], out.at[:, y, x, core, b_rows]
            items = [(a, a, y_peer), (b, b, x_peer)]
        elif phase == 2:
            a, b = out.at[:, :, x, core, a_rows], out.at[:, y, :, core, b_rows]
            items = [(a, a, x_peer), (b, b, y_peer)]
        else:
            a = out.at[:, :, :, core, all_rows]
            items = [(a, a, partner)]
        base = (0, 3, 5, 7)[phase]
        return [remote(s, d, send.at[par, i, base + k], recv.at[par, i, base + k], dev) for k, (s, d, dev) in enumerate(items)]

    for tick in range(n_chunks + 3):
        live = []
        for phase in (2, 1, 0, 3):
            chunk = tick - phase
            if 0 <= chunk < n_chunks:
                for i in range(n_arr):
                    live += phase_copies(chunk, phase, tick % 2, i)
        for copy in live:
            copy.start()
        for copy in live:
            copy.wait()


def gather_rows(mats, collective_id):
    n_arr = len(mats)
    outs = pl.pallas_call(
        functools.partial(gather_rows_kernel, n_arr),
        out_shape=[jax.ShapeDtypeStruct((4, 2, 2, 2) + m.shape, m.dtype) for m in mats],
        in_specs=[pl.BlockSpec(memory_space=pltpu.VMEM)] * n_arr,
        out_specs=[pl.BlockSpec(memory_space=pl.ANY)] * n_arr,
        scratch_shapes=[
            pltpu.SemaphoreType.DMA((2, n_arr, 8)),
            pltpu.SemaphoreType.DMA((2, n_arr, 8)),
            pltpu.SemaphoreType.DMA((n_arr,)),
        ],
        compiler_params=pltpu.CompilerParams(collective_id=collective_id, has_side_effects=True),
        name='gather_rows',
    )(*mats)
    return [o.reshape(32 * m.shape[0], m.shape[1]) for o, m in zip(outs, mats)]


def mlp_kernel(u, dout, zg, zu, dmd, zg_t, zu_t, dmd_t, w_loc, b_gate, b_up, a_down_t, w_down,
               down_out, back_out, z_down, dm_gate, dm_up, gb_gate, gb_up, ga_down_t, full,
               w_gu, w_dn, send, recv, own_sem, load_sem):
    n_chunks = w_loc.shape[0]
    half = w_loc.shape[2] // 2
    width = w_loc.shape[3]
    rows = 32 * w_loc.shape[2]
    me, z, y, x, core = coords()
    z_peers, y_peer, x_peer, partner = peers(me, z, y, x, core)
    entry_barrier(z_peers + [y_peer, x_peer, partner])
    a_rows, b_rows = pl.ds(0, half), pl.ds(half, half)

    own = pltpu.make_async_copy(w_loc, full.at[:, :, z, y, x, core], own_sem)
    own.start()
    own.wait()

    def phase_copies(chunk, phase, par):
        if phase == 0:
            items = [(w_loc.at[chunk], full.at[chunk, :, z, y, x, core], dev) for dev in z_peers]
        elif phase == 1:
            a, b = full.at[chunk, :, :, y, x, core, a_rows], full.at[chunk, :, :, y, x, core, b_rows]
            items = [(a, a, y_peer), (b, b, x_peer)]
        elif phase == 2:
            a, b = full.at[chunk, :, :, :, x, core, a_rows], full.at[chunk, :, :, y, :, core, b_rows]
            items = [(a, a, x_peer), (b, b, y_peer)]
        else:
            a = full.at[chunk, :, :, :, :, core]
            items = [(a, a, partner)]
        base = (0, 3, 5, 7)[phase]
        return [remote(s, d, send.at[par, base + k], recv.at[par, base + k], dev) for k, (s, d, dev) in enumerate(items)]

    down_out[...] = jnp.zeros_like(down_out)
    back_out[...] = jnp.zeros_like(back_out)
    z_down[...] = jnp.zeros_like(z_down)
    dm_gate[...] = jnp.zeros_like(dm_gate)
    dm_up[...] = jnp.zeros_like(dm_up)

    def loads(chunk):
        at = pl.multiple_of(chunk * width, width)
        return (pltpu.make_async_copy(full.at[chunk, 0], w_gu.at[0], load_sem.at[0]),
                pltpu.make_async_copy(full.at[chunk, 1], w_gu.at[1], load_sem.at[1]),
                pltpu.make_async_copy(w_down.at[pl.ds(at, width), :], w_dn, load_sem.at[2]))

    def compute(chunk):
        at = pl.multiple_of(chunk * width, width)
        cols = pl.ds(at, width)
        load_g, load_u, load_d = loads(chunk)
        load_g.start()
        load_u.start()
        load_d.start()
        bg, bu, ad = b_gate[:, cols], b_up[:, cols], a_down_t[:, cols]
        load_g.wait()
        wg = w_gu[0].reshape(rows, width)
        gate = dot_nn(u[...], wg) + LORA_SCALE * dot_nn(zg[...], bg)
        load_u.wait()
        wu = w_gu[1].reshape(rows, width)
        up = dot_nn(u[...], wu) + LORA_SCALE * dot_nn(zu[...], bu)
        sig = jax.nn.sigmoid(gate)
        silu = gate * sig
        act = (silu * up).astype(BF16)
        load_d.wait()
        grad_act = (dot_nt(dout[...], w_dn[...]) + dot_nn(dmd[...], ad)).astype(BF16).astype(F32)
        d_up = grad_act * silu
        d_gate = grad_act * up * (sig + silu * (1.0 - sig))
        down_out[...] += dot_nn(act, w_dn[...])
        z_down[...] += dot_nt(act.astype(F32), ad)
        ga_down_t[:, cols] = dot_nn(dmd_t[...], act.astype(F32))
        gb_gate[:, cols] = LORA_SCALE * dot_nn(zg_t[...], d_gate)
        gb_up[:, cols] = LORA_SCALE * dot_nn(zu_t[...], d_up)
        dm_gate[...] += LORA_SCALE * dot_nt(d_gate, bg)
        dm_up[...] += LORA_SCALE * dot_nt(d_up, bu)
        back_out[...] += dot_nt(d_gate.astype(BF16), wg) + dot_nt(d_up.astype(BF16), wu)

    def tick_body(tick, carry):
        par = lax.rem(tick, 2)
        for phase in (2, 1, 0, 3):
            chunk = tick - phase

            @pl.when((chunk >= 0) & (chunk < n_chunks))
            def _(chunk=chunk, phase=phase):
                for copy in phase_copies(chunk, phase, par):
                    copy.start()

        @pl.when(tick >= 4)
        def _():
            compute(tick - 4)

        for phase in (2, 1, 0, 3):
            chunk = tick - phase

            @pl.when((chunk >= 0) & (chunk < n_chunks))
            def _(chunk=chunk, phase=phase):
                for copy in phase_copies(chunk, phase, par):
                    copy.wait()
        return carry

    lax.fori_loop(0, n_chunks + 4, tick_body, 0)


def fused_mlp(u, dout, zg, zu, dmd, w_gate, w_up, b_gate, b_up, a_down_t, w_down, collective_id):
    tokens, model_dim = u.shape
    shard, ff = w_gate.shape
    rank = zg.shape[1]
    n_chunks = ff // FF_CHUNK
    w_loc = jnp.stack([w_gate, w_up]).reshape(2, shard, n_chunks, FF_CHUNK).transpose(2, 0, 1, 3)
    vmem = pl.BlockSpec(memory_space=pltpu.VMEM)
    hbm = pl.BlockSpec(memory_space=pl.ANY)
    f32 = lambda *s: jax.ShapeDtypeStruct(s, F32)
    outs = pl.pallas_call(
        mlp_kernel,
        out_shape=[f32(tokens, model_dim), f32(tokens, model_dim), f32(tokens, rank), f32(tokens, rank), f32(tokens, rank),
                   f32(rank, ff), f32(rank, ff), f32(rank, ff),
                   jax.ShapeDtypeStruct((n_chunks, 2, 4, 2, 2, 2, shard, FF_CHUNK), BF16)],
        in_specs=[vmem] * 12 + [hbm],
        out_specs=[vmem] * 8 + [hbm],
        scratch_shapes=[
            pltpu.VMEM((2, 4, 2, 2, 2, shard, FF_CHUNK), BF16),
            pltpu.VMEM((FF_CHUNK, model_dim), BF16),
            pltpu.SemaphoreType.DMA((2, 8)),
            pltpu.SemaphoreType.DMA((2, 8)),
            pltpu.SemaphoreType.DMA,
            pltpu.SemaphoreType.DMA((3,)),
        ],
        compiler_params=pltpu.CompilerParams(collective_id=collective_id, has_side_effects=True, vmem_limit_bytes=60 * 2 ** 20),
        cost_estimate=pl.CostEstimate(flops=12 * tokens * model_dim * ff, bytes_accessed=6 * model_dim * ff, transcendentals=0),
        name='fused_mlp',
    )(u, dout, zg, zu, dmd, zg.T, zu.T, dmd.T, w_loc, b_gate, b_up, a_down_t, w_down)
    return outs[:8]


def layer_step(hidden, grad_next, seq_len, gain_attn, gain_mlp, base_shards, lora):
    w_q, w_k, w_v, w_o, w_gate, w_up, w_down = base_shards
    a_q, b_q, a_k, b_k, a_v, b_v, a_o, b_o, a_gate, b_gate, a_up, b_up, a_down, b_down = lora
    tokens, model_dim = hidden.shape
    n_seq = tokens // seq_len
    shard = w_q.shape[0]
    n_heads, head_dim = w_q.shape[1:]
    kv_heads = w_k.shape[1]
    q_dim, k_dim = n_heads * head_dim, kv_heads * head_dim
    rank = a_q.shape[1]
    w_qkv_loc = jnp.concatenate([w_q.reshape(shard, q_dim), w_k.reshape(shard, k_dim), w_v.reshape(shard, k_dim)], axis=1)
    w_qkv, w_o_full = gather_rows([w_qkv_loc, w_o], 0)
    w_down_full = lax.all_gather(w_down, AXIS, axis=0, tiled=True)

    normed, norm_attn_pull = jax.vjp(lambda h: rms_norm(h, gain_attn), hidden)
    a_qkv = jnp.concatenate([a_q, a_k, a_v], axis=1)
    z_qkv = jnp.dot(normed, a_qkv, preferred_element_type=F32)
    z_q, z_k, z_v = z_qkv[:, :rank], z_qkv[:, rank:2 * rank], z_qkv[:, 2 * rank:]
    qkv = dot_nn(normed, w_qkv)
    q_flat = qkv[:, :q_dim] + LORA_SCALE * dot_nn(z_q, b_q)
    k_flat = qkv[:, q_dim:q_dim + k_dim] + LORA_SCALE * dot_nn(z_k, b_k)
    v_flat = qkv[:, q_dim + k_dim:] + LORA_SCALE * dot_nn(z_v, b_v)
    q_proj = q_flat.reshape(n_seq, seq_len, n_heads, head_dim)
    k_proj = k_flat.reshape(n_seq, seq_len, kv_heads, head_dim)
    v_proj = v_flat.astype(BF16).reshape(n_seq, seq_len, kv_heads, head_dim)
    attn_out, attn_pull = jax.vjp(attn_core, q_proj, k_proj, v_proj)
    z_o = jnp.dot(attn_out, a_o, preferred_element_type=F32)
    o_full = dot_nn(attn_out, w_o_full) + LORA_SCALE * dot_nn(z_o, b_o)
    h_mid = (hidden.astype(F32) + o_full).astype(BF16)
    normed_mlp, norm_mlp_pull = jax.vjp(lambda h: rms_norm(h, gain_mlp), h_mid)

    z_gu = jnp.dot(normed_mlp, jnp.concatenate([a_gate, a_up], axis=1), preferred_element_type=F32)
    z_gate, z_up = z_gu[:, :rank], z_gu[:, rank:]
    dmid_down = LORA_SCALE * dot_nt(grad_next.astype(F32), b_down)
    down_out, back, z_down, dmid_gate, dmid_up, g_b_gate, g_b_up, g_a_down_t = fused_mlp(
        normed_mlp, grad_next, z_gate, z_up, dmid_down, w_gate, w_up, b_gate, b_up, a_down.T, w_down_full, 1)
    hidden_next = (h_mid.astype(F32) + down_out + LORA_SCALE * dot_nn(z_down, b_down)).astype(BF16)
    g_b_down = LORA_SCALE * dot_tn(z_down, grad_next.astype(F32))
    g_a_gate = dot_tn(normed_mlp.astype(F32), dmid_gate)
    g_a_up = dot_tn(normed_mlp.astype(F32), dmid_up)
    mlp_grads = lax.psum((g_a_gate, g_b_gate, g_a_up, g_b_up, g_a_down_t, g_b_down), AXIS)
    back = back + dot_nt(dmid_gate, a_gate) + dot_nt(dmid_up, a_up)
    grad_norm_mlp = norm_mlp_pull(back.astype(BF16))[0]
    grad_mid = (grad_next.astype(F32) + grad_norm_mlp.astype(F32)).astype(BF16)

    grad_mid_f32 = grad_mid.astype(F32)
    dmid_o = LORA_SCALE * dot_nt(grad_mid_f32, b_o)
    grad_attn = dot_nt(grad_mid, w_o_full) + dot_nt(dmid_o, a_o)
    g_a_o = dot_tn(attn_out.astype(F32), dmid_o)
    g_b_o = LORA_SCALE * dot_tn(z_o, grad_mid_f32)
    grad_q, grad_k, grad_v = attn_pull(grad_attn.astype(BF16))
    grad_q = grad_q.reshape(tokens, -1).astype(F32)
    grad_k = grad_k.reshape(tokens, -1).astype(F32)
    grad_v = grad_v.reshape(tokens, -1).astype(F32)
    normed_f32 = normed.astype(F32)
    dmids = []
    bs = []
    for z_mid, grad_y, b_mat in ((z_q, grad_q, b_q), (z_k, grad_k, b_k), (z_v, grad_v, b_v)):
        dmids.append(LORA_SCALE * dot_nt(grad_y, b_mat))
        bs.append(LORA_SCALE * dot_tn(z_mid, grad_y))
    g_a_qkv = dot_tn(normed_f32, jnp.concatenate(dmids, axis=1))
    g_a_q, g_a_k, g_a_v = g_a_qkv[:, :rank], g_a_qkv[:, rank:2 * rank], g_a_qkv[:, 2 * rank:]
    attn_local, mlp_grads = lax.optimization_barrier(((g_a_q, bs[0], g_a_k, bs[1], g_a_v, bs[2], g_a_o, g_b_o), mlp_grads))
    attn_grads = lax.psum(attn_local, AXIS)
    g_a_gate, g_b_gate, g_a_up, g_b_up, g_a_down_t, g_b_down = mlp_grads
    return hidden_next, attn_grads + (g_a_gate, g_b_gate, g_a_up, g_b_up, g_a_down_t.T, g_b_down)


def solution(mesh):
    tok_spec = P(AXIS)
    row_spec = P(None, AXIS)
    rep_spec = P()
    in_specs = (tok_spec, tok_spec, rep_spec, rep_spec) + (row_spec,) * 7 + (rep_spec,) * 14
    out_specs = (tok_spec,) + (rep_spec,) * 14

    def per_device(hidden_in, grad_out, gain_attn, gain_mlp, *weights):
        n_seq, seq_len, model_dim = hidden_in.shape
        base = tuple(w[0] for w in weights[:7])
        lora = tuple(w[0] for w in weights[7:])
        hidden_next, grads = layer_step(hidden_in.reshape(-1, model_dim), grad_out.reshape(-1, model_dim), seq_len,
                                        gain_attn[0], gain_mlp[0], base, lora)
        return (hidden_next.reshape(hidden_in.shape),) + tuple(g[None] for g in grads)

    return jax.shard_map(per_device, mesh=mesh, in_specs=in_specs, out_specs=out_specs, check_vma=False)
```

```python
import functools

import jax
import jax.numpy as jnp
from jax import lax
from jax.experimental import pallas as pl
from jax.experimental.pallas import tpu as pltpu
from jax.sharding import PartitionSpec as P

LORA_SCALE = 2.0
NORM_EPS = 1e-5
ROPE_BASE = 10000.0
AXIS = 'fsdp'
F32 = jnp.float32
BF16 = jnp.bfloat16
FF_CHUNK = 256
DOWN_COLS = 512
N_SPANS = 4


def rms_norm(hidden, gain_vec):
    hid_f32 = hidden.astype(F32)
    inv_rms = lax.rsqrt(jnp.mean(hid_f32 * hid_f32, axis=-1, keepdims=True) + NORM_EPS)
    return (hid_f32 * inv_rms * gain_vec.astype(F32)).astype(BF16)


def apply_rope(rot_in):
    seq_len, head_dim = rot_in.shape[1], rot_in.shape[3]
    half_dim = head_dim // 2
    inv_freq = ROPE_BASE ** (-jnp.arange(half_dim, dtype=F32) * 2.0 / head_dim)
    angles = jnp.arange(seq_len, dtype=F32)[:, None] * inv_freq[None, :]
    cos_t = jnp.cos(angles)[:, None, :]
    sin_t = jnp.sin(angles)[:, None, :]
    first_half = rot_in[..., :half_dim]
    second_half = rot_in[..., half_dim:]
    return jnp.concatenate([first_half * cos_t - second_half * sin_t, second_half * cos_t + first_half * sin_t], axis=-1)


def attn_core(q_proj, k_proj, v_proj):
    n_seq, seq_len, n_heads, head_dim = q_proj.shape
    kv_heads = k_proj.shape[2]
    q_rot = apply_rope(q_proj).astype(BF16).reshape(n_seq, seq_len, kv_heads, n_heads // kv_heads, head_dim)
    k_rot = apply_rope(k_proj).astype(BF16)
    scores = jnp.einsum('bqkgd,bskd->bkgqs', q_rot, k_rot, preferred_element_type=F32) * (head_dim ** -0.5)
    causal = jnp.arange(seq_len)[:, None] >= jnp.arange(seq_len)[None, :]
    attn_probs = jax.nn.softmax(jnp.where(causal, scores, -1e30), axis=-1).astype(BF16)
    attn_out = jnp.einsum('bkgqs,bskd->bqkgd', attn_probs, v_proj, preferred_element_type=F32)
    return attn_out.astype(BF16).reshape(n_seq * seq_len, n_heads * head_dim)


def dot_nn(a, b):
    return lax.dot_general(a, b, (((1,), (0,)), ((), ())), preferred_element_type=F32)


def dot_nt(a, b):
    return lax.dot_general(a, b, (((1,), (1,)), ((), ())), preferred_element_type=F32)


def dot_tn(a, b):
    return lax.dot_general(a, b, (((0,), (0,)), ((), ())), preferred_element_type=F32)


def coords():
    me = lax.axis_index(AXIS)
    core = lax.rem(me, 2)
    x = lax.rem(me // 2, 2)
    y = lax.rem(me // 4, 2)
    z = me // 8
    return me, z, y, x, core


def peers(me, z, y, x, core):
    z_peers = [me + 8 * (lax.rem(z + k, 4) - z) for k in (1, 2, 3)]
    return z_peers, me + 4 * (1 - 2 * y), me + 2 * (1 - 2 * x), me + 1 - 2 * core


def entry_barrier(devices):
    barrier = pltpu.get_barrier_semaphore()
    for dev in devices:
        pl.semaphore_signal(barrier, inc=1, device_id=(dev,), device_id_type=pl.DeviceIdType.MESH)
    pl.semaphore_wait(barrier, len(devices))


def remote(src, dst, send_sem, recv_sem, dev):
    return pltpu.make_async_remote_copy(src_ref=src, dst_ref=dst, send_sem=send_sem, recv_sem=recv_sem,
                                        device_id=(dev,), device_id_type=pl.DeviceIdType.MESH)


N_COPIES = 14


def gather_phase(src, out, phase, row, n_rows, send, recv):
    me, z, y, x, core = coords()
    z_peers, y_peer, x_peer, partner = peers(me, z, y, x, core)
    tiles = n_rows // 8
    n_c = tiles // 8
    n_a = (tiles - n_c + 1) // 2
    n_b = tiles - n_c - n_a
    a_rows = pl.ds(row, 8 * n_a)
    b_rows = pl.ds(row + 8 * n_a, 8 * n_b)
    ab_rows = pl.ds(row, 8 * (n_a + n_b))
    c_rows = pl.ds(row + 8 * (n_a + n_b), 8 * n_c)
    if phase == 0:
        items = [(src.at[ab_rows], out.at[z, y, x, core, ab_rows], dev) for dev in z_peers]
        if n_c:
            items.append((src.at[c_rows], out.at[z, y, x, core, c_rows], x_peer))
    elif phase == 1:
        items = [(out.at[:, y, x, core, a_rows], y_peer), (out.at[:, y, x, core, b_rows], x_peer)]
        if n_c:
            items.append((out.at[z, y, :, core, c_rows], y_peer))
    elif phase == 2:
        items = [(out.at[:, :, x, core, a_rows], x_peer), (out.at[:, y, :, core, b_rows], y_peer)]
        if n_c:
            items += [(out.at[z, :, :, core, c_rows], dev) for dev in z_peers]
    else:
        items = [(out.at[:, :, :, core, pl.ds(row, n_rows)], partner)]
    base = (0, 4, 7, 12)[phase]
    copies = []
    for k, item in enumerate(items):
        s_ref, d_ref, dev = item if len(item) == 3 else (item[0],) + item
        copies.append(remote(s_ref, d_ref, send.at[base + k], recv.at[base + k], dev))
    return copies


def gather_rows_kernel(n_arr, *refs):
    srcs, outs = refs[:n_arr], refs[n_arr:2 * n_arr]
    send, recv, own_sem = refs[2 * n_arr:]
    me, z, y, x, core = coords()
    z_peers, y_peer, x_peer, partner = peers(me, z, y, x, core)
    entry_barrier(z_peers + [y_peer, x_peer, partner])
    def own_copy(i):
        return pltpu.make_async_copy(srcs[i], outs[i].at[z, y, x, core], own_sem.at[i])

    for i in range(n_arr):
        own_copy(i).start()
    for i in range(n_arr):
        own_copy(i).wait()

    spans = []
    for src in srcs:
        rows = src.shape[0]
        step = -(-rows // (8 * N_SPANS)) * 8
        spans.append([(at, min(step, rows - at)) for at in range(0, rows, step)])
    n_ticks = max(len(s) for s in spans)

    def tick_copies(tick, i):
        live = []
        for phase in (2, 1, 0, 3):
            if 0 <= tick - phase < len(spans[i]):
                row, n_rows = spans[i][tick - phase]
                live += gather_phase(srcs[i], outs[i], phase, row, n_rows, send.at[tick % 2, i], recv.at[tick % 2, i])
        return live

    for tick in range(n_ticks + 4):
        for i in range(n_arr):
            for copy in tick_copies(tick - 1, i):
                copy.wait()
            for copy in tick_copies(tick, i):
                copy.start()


def gather_rows(mats, collective_id):
    n_arr = len(mats)
    outs = pl.pallas_call(
        functools.partial(gather_rows_kernel, n_arr),
        out_shape=[jax.ShapeDtypeStruct((4, 2, 2, 2) + m.shape, m.dtype) for m in mats],
        in_specs=[pl.BlockSpec(memory_space=pltpu.VMEM)] * n_arr,
        out_specs=[pl.BlockSpec(memory_space=pl.ANY)] * n_arr,
        scratch_shapes=[
            pltpu.SemaphoreType.DMA((2, n_arr, N_COPIES)),
            pltpu.SemaphoreType.DMA((2, n_arr, N_COPIES)),
            pltpu.SemaphoreType.DMA((n_arr,)),
        ],
        compiler_params=pltpu.CompilerParams(collective_id=collective_id, has_side_effects=True),
        name='gather_rows',
    )(*mats)
    return [o.reshape(32 * m.shape[0], m.shape[1]) for o, m in zip(outs, mats)]


def all_reduce_kernel(x_in, out, acc, r_core, r2a, r2b, r3a, r3b, r4, send, recv):
    me, z, y, x, core = coords()
    z_peers, y_peer, x_peer, partner = peers(me, z, y, x, core)
    entry_barrier(z_peers + [y_peer, x_peer, partner])
    block = x_in.shape[3] // 4
    wide = r3a.shape[2]

    def cols(yy, xx):
        return pl.ds(pl.multiple_of((yy * 2 + xx) * block, 128), block)

    def cols_a(yy, xx):
        return pl.ds(pl.multiple_of((yy * 2 + xx) * block, 128), wide)

    def cols_b(yy, xx):
        return pl.ds(pl.multiple_of((yy * 2 + xx) * block + wide, 128), block - wide)

    used = [0]

    def exchange(items):
        copies = []
        for src, dst, dev in items:
            copies.append(remote(src, dst, send.at[used[0]], recv.at[used[0]], dev))
            used[0] += 1
        for copy in copies:
            copy.start()
        for copy in copies:
            copy.wait()

    exchange([(x_in.at[1 - core], r_core, partner)])
    acc[...] = x_in[core] + r_core[...]
    exchange([(acc.at[:, :, cols_a(i, 1 - x)], r2a.at[i], x_peer) for i in range(2)]
             + [(acc.at[:, :, cols_b(1 - y, i)], r2b.at[i], y_peer) for i in range(2)])
    for i in range(2):
        acc[:, :, cols_a(i, x)] += r2a[i]
        acc[:, :, cols_b(y, i)] += r2b[i]
    exchange([(acc.at[:, :, cols_a(1 - y, x)], r3a, y_peer), (acc.at[:, :, cols_b(y, 1 - x)], r3b, x_peer)])
    acc[:, :, cols_a(y, x)] += r3a[...]
    acc[:, :, cols_b(y, x)] += r3b[...]
    here = cols(y, x)
    exchange([(acc.at[lax.rem(z + k + 1, 4), :, here], r4.at[k], z_peers[k]) for k in range(3)])
    out[core, z, :, here] = acc[z, :, here] + (r4[0] + r4[1] + r4[2])
    exchange([(out.at[core, z, :, here], out.at[core, z, :, here], dev) for dev in z_peers])

    def same(at, dev):
        ref = out.at[core, :, :, at]
        return ref, ref, dev

    exchange([same(cols_a(y, x), y_peer), same(cols_b(y, x), x_peer)])
    exchange([same(cols_a(i, x), x_peer) for i in range(2)] + [same(cols_b(y, i), y_peer) for i in range(2)])
    exchange([(out.at[core], out.at[core], partner)])


def all_reduce_rows(x, collective_id):
    n = x.shape[1]
    block = n // 4
    wide = (block // 256 + (block // 128) % 2) * 128
    vmem = pl.BlockSpec(memory_space=pltpu.VMEM)
    out = pl.pallas_call(
        all_reduce_kernel,
        out_shape=jax.ShapeDtypeStruct((2, 4, 8, n), F32),
        in_specs=[vmem],
        out_specs=vmem,
        scratch_shapes=[
            pltpu.VMEM((4, 8, n), F32),
            pltpu.VMEM((4, 8, n), F32),
            pltpu.VMEM((2, 4, 8, wide), F32),
            pltpu.VMEM((2, 4, 8, block - wide), F32),
            pltpu.VMEM((4, 8, wide), F32),
            pltpu.VMEM((4, 8, block - wide), F32),
            pltpu.VMEM((3, 8, block), F32),
            pltpu.SemaphoreType.DMA((20,)),
            pltpu.SemaphoreType.DMA((20,)),
        ],
        compiler_params=pltpu.CompilerParams(collective_id=collective_id, has_side_effects=True),
        name='all_reduce_rows',
    )(x.reshape(2, 4, 8, n))
    return out.reshape(64, n)


def mlp_kernel(u, dout, zg, zu, dmd, zg_t, zu_t, dmd_t, w_loc, b_gate, b_up, a_down_t, w_down_a, w_down_b,
               down_out, back_out, z_down, dm_gate, dm_up, gb_gate, gb_up, ga_down_t, full,
               w_gu, w_dn, send, recv, own_sem, load_sem):
    n_chunks = w_loc.shape[0]
    width = w_loc.shape[3]
    rows = 32 * w_loc.shape[2]
    me, z, y, x, core = coords()
    z_peers, y_peer, x_peer, partner = peers(me, z, y, x, core)
    entry_barrier(z_peers + [y_peer, x_peer, partner])
    own = pltpu.make_async_copy(w_loc, full.at[:, :, z, y, x, core], own_sem)
    own.start()
    own.wait()

    def phase_copies(chunk, phase, par, part):
        return gather_phase(w_loc.at[chunk, part], full.at[chunk, part], phase, 0, w_loc.shape[2],
                            send.at[par, part], recv.at[par, part])

    down_out[...] = jnp.zeros_like(down_out)
    back_out[...] = jnp.zeros_like(back_out)
    z_down[...] = jnp.zeros_like(z_down)
    dm_gate[...] = jnp.zeros_like(dm_gate)
    dm_up[...] = jnp.zeros_like(dm_up)

    def loads(chunk):
        at = pl.multiple_of(chunk * width, width)
        return (pltpu.make_async_copy(full.at[chunk, 0], w_gu.at[0], load_sem.at[0]),
                pltpu.make_async_copy(full.at[chunk, 1], w_gu.at[1], load_sem.at[1]),
                pltpu.make_async_copy(w_down_a.at[pl.ds(at, width), :], w_dn.at[:, pl.ds(0, DOWN_COLS)], load_sem.at[2]),
                pltpu.make_async_copy(w_down_b.at[pl.ds(at, width), :], w_dn.at[:, pl.ds(DOWN_COLS, w_dn.shape[1] - DOWN_COLS)], load_sem.at[3]))

    def compute(chunk):
        at = pl.multiple_of(chunk * width, width)
        cols = pl.ds(at, width)
        load_g, load_u, load_a, load_b = loads(chunk)
        load_g.start()
        load_u.start()
        load_a.start()
        load_b.start()
        bg, bu, ad = b_gate[:, cols], b_up[:, cols], a_down_t[:, cols]
        load_g.wait()
        wg = w_gu[0].reshape(rows, width)
        gate = dot_nn(u[...], wg) + LORA_SCALE * dot_nn(zg[...], bg)
        load_u.wait()
        wu = w_gu[1].reshape(rows, width)
        up = dot_nn(u[...], wu) + LORA_SCALE * dot_nn(zu[...], bu)
        sig = jax.nn.sigmoid(gate)
        silu = gate * sig
        act = (silu * up).astype(BF16)
        load_a.wait()
        load_b.wait()
        grad_act = (dot_nt(dout[...], w_dn[...]) + dot_nn(dmd[...], ad)).astype(BF16).astype(F32)
        d_up = grad_act * silu
        d_gate = grad_act * up * (sig + silu * (1.0 - sig))
        down_out[...] += dot_nn(act, w_dn[...])
        z_down[...] += dot_nt(act.astype(F32), ad)
        ga_down_t[:, cols] = dot_nn(dmd_t[...], act.astype(F32))
        gb_gate[:, cols] = LORA_SCALE * dot_nn(zg_t[...], d_gate)
        gb_up[:, cols] = LORA_SCALE * dot_nn(zu_t[...], d_up)
        dm_gate[...] += LORA_SCALE * dot_nt(d_gate, bg)
        dm_up[...] += LORA_SCALE * dot_nt(d_up, bu)
        back_out[...] += dot_nt(d_gate.astype(BF16), wg) + dot_nt(d_up.astype(BF16), wu)

    def each_copy(tick, part, act):
        par = lax.rem(tick + 2, 2)
        for phase in (2, 1, 0, 3):
            chunk = tick - phase

            @pl.when((chunk >= 0) & (chunk < n_chunks))
            def _(chunk=chunk, phase=phase):
                for copy in phase_copies(chunk, phase, par, part):
                    act(copy)

    def tick_body(tick, carry):
        for part in range(2):
            each_copy(tick - 1, part, lambda copy: copy.wait())
            each_copy(tick, part, lambda copy: copy.start())

        @pl.when(tick >= 4)
        def _():
            compute(tick - 4)
        return carry

    lax.fori_loop(0, n_chunks + 4, tick_body, 0)


def fused_mlp(u, dout, zg, zu, dmd, w_gate, w_up, b_gate, b_up, a_down_t, w_down_a, w_down_b, collective_id):
    tokens, model_dim = u.shape
    shard, ff = w_gate.shape
    rank = zg.shape[1]
    n_chunks = ff // FF_CHUNK
    w_loc = jnp.stack([w_gate, w_up]).reshape(2, shard, n_chunks, FF_CHUNK).transpose(2, 0, 1, 3)
    vmem = pl.BlockSpec(memory_space=pltpu.VMEM)
    hbm = pl.BlockSpec(memory_space=pl.ANY)
    f32 = lambda *s: jax.ShapeDtypeStruct(s, F32)
    outs = pl.pallas_call(
        mlp_kernel,
        out_shape=[f32(tokens, model_dim), f32(tokens, model_dim), f32(tokens, rank), f32(tokens, rank), f32(tokens, rank),
                   f32(rank, ff), f32(rank, ff), f32(rank, ff),
                   jax.ShapeDtypeStruct((n_chunks, 2, 4, 2, 2, 2, shard, FF_CHUNK), BF16)],
        in_specs=[vmem] * 12 + [hbm] * 2,
        out_specs=[vmem] * 8 + [hbm],
        scratch_shapes=[
            pltpu.VMEM((2, 4, 2, 2, 2, shard, FF_CHUNK), BF16),
            pltpu.VMEM((FF_CHUNK, model_dim), BF16),
            pltpu.SemaphoreType.DMA((2, 2, N_COPIES)),
            pltpu.SemaphoreType.DMA((2, 2, N_COPIES)),
            pltpu.SemaphoreType.DMA,
            pltpu.SemaphoreType.DMA((4,)),
        ],
        compiler_params=pltpu.CompilerParams(collective_id=collective_id, has_side_effects=True, vmem_limit_bytes=60 * 2 ** 20),
        cost_estimate=pl.CostEstimate(flops=12 * tokens * model_dim * ff, bytes_accessed=6 * model_dim * ff, transcendentals=0),
        name='fused_mlp',
    )(u, dout, zg, zu, dmd, zg.T, zu.T, dmd.T, w_loc, b_gate, b_up, a_down_t, w_down_a, w_down_b)
    return outs[:8]


def layer_step(hidden, grad_next, seq_len, gain_attn, gain_mlp, base_shards, lora):
    w_q, w_k, w_v, w_o, w_gate, w_up, w_down = base_shards
    a_q, b_q, a_k, b_k, a_v, b_v, a_o, b_o, a_gate, b_gate, a_up, b_up, a_down, b_down = lora
    tokens, model_dim = hidden.shape
    n_seq = tokens // seq_len
    shard = w_q.shape[0]
    n_heads, head_dim = w_q.shape[1:]
    kv_heads = w_k.shape[1]
    q_dim, k_dim = n_heads * head_dim, kv_heads * head_dim
    rank = a_q.shape[1]
    w_qkv_loc = jnp.concatenate([w_q.reshape(shard, q_dim), w_k.reshape(shard, k_dim), w_v.reshape(shard, k_dim)], axis=1)
    w_half = w_qkv_loc.shape[1] // 2
    w_qkv_a, w_qkv_b, w_down_a = gather_rows([w_qkv_loc[:, :w_half], w_qkv_loc[:, w_half:], w_down[:, :DOWN_COLS]], 0)
    w_o_full = lax.all_gather(w_o, AXIS, axis=0, tiled=True)
    w_down_b = lax.all_gather(w_down[:, DOWN_COLS:], AXIS, axis=0, tiled=True)

    normed, norm_attn_pull = jax.vjp(lambda h: rms_norm(h, gain_attn), hidden)
    a_qkv = jnp.concatenate([a_q, a_k, a_v], axis=1)
    z_qkv = jnp.dot(normed, a_qkv, preferred_element_type=F32)
    z_q, z_k, z_v = z_qkv[:, :rank], z_qkv[:, rank:2 * rank], z_qkv[:, 2 * rank:]
    qkv = jnp.concatenate([dot_nn(normed, w_qkv_a), dot_nn(normed, w_qkv_b)], axis=1)
    q_flat = qkv[:, :q_dim] + LORA_SCALE * dot_nn(z_q, b_q)
    k_flat = qkv[:, q_dim:q_dim + k_dim] + LORA_SCALE * dot_nn(z_k, b_k)
    v_flat = qkv[:, q_dim + k_dim:] + LORA_SCALE * dot_nn(z_v, b_v)
    q_proj = q_flat.reshape(n_seq, seq_len, n_heads, head_dim)
    k_proj = k_flat.reshape(n_seq, seq_len, kv_heads, head_dim)
    v_proj = v_flat.astype(BF16).reshape(n_seq, seq_len, kv_heads, head_dim)
    attn_out, attn_pull = jax.vjp(attn_core, q_proj, k_proj, v_proj)
    z_o = jnp.dot(attn_out, a_o, preferred_element_type=F32)
    o_full = dot_nn(attn_out, w_o_full) + LORA_SCALE * dot_nn(z_o, b_o)
    h_mid = (hidden.astype(F32) + o_full).astype(BF16)
    normed_mlp, norm_mlp_pull = jax.vjp(lambda h: rms_norm(h, gain_mlp), h_mid)

    z_gu = jnp.dot(normed_mlp, jnp.concatenate([a_gate, a_up], axis=1), preferred_element_type=F32)
    z_gate, z_up = z_gu[:, :rank], z_gu[:, rank:]
    dmid_down = LORA_SCALE * dot_nt(grad_next.astype(F32), b_down)
    down_out, back, z_down, dmid_gate, dmid_up, g_b_gate, g_b_up, g_a_down_t = fused_mlp(
        normed_mlp, grad_next, z_gate, z_up, dmid_down, w_gate, w_up, b_gate, b_up, a_down.T, w_down_a, w_down_b, 1)
    hidden_next = (h_mid.astype(F32) + down_out + LORA_SCALE * dot_nn(z_down, b_down)).astype(BF16)
    g_b_down = LORA_SCALE * dot_tn(z_down, grad_next.astype(F32))
    g_a_gate = dot_tn(normed_mlp.astype(F32), dmid_gate)
    g_a_up = dot_tn(normed_mlp.astype(F32), dmid_up)
    mlp_grads = lax.psum((g_a_gate, g_b_gate, g_a_up, g_b_up, g_a_down_t, g_b_down), AXIS)
    back = back + dot_nt(dmid_gate, a_gate) + dot_nt(dmid_up, a_up)
    grad_norm_mlp = norm_mlp_pull(back.astype(BF16))[0]
    grad_mid = (grad_next.astype(F32) + grad_norm_mlp.astype(F32)).astype(BF16)

    grad_mid_f32 = grad_mid.astype(F32)
    dmid_o = LORA_SCALE * dot_nt(grad_mid_f32, b_o)
    grad_attn = dot_nt(grad_mid, w_o_full) + dot_nt(dmid_o, a_o)
    g_at_o = dot_tn(dmid_o, attn_out.astype(F32))
    g_b_o = LORA_SCALE * dot_tn(z_o, grad_mid_f32)
    grad_q, grad_k, grad_v = attn_pull(grad_attn.astype(BF16))
    grad_q = grad_q.reshape(tokens, -1).astype(F32)
    grad_k = grad_k.reshape(tokens, -1).astype(F32)
    grad_v = grad_v.reshape(tokens, -1).astype(F32)
    normed_f32 = normed.astype(F32)
    dmids = []
    bs = []
    for z_mid, grad_y, b_mat in ((z_q, grad_q, b_q), (z_k, grad_k, b_k), (z_v, grad_v, b_v)):
        dmids.append(LORA_SCALE * dot_nt(grad_y, b_mat))
        bs.append(LORA_SCALE * dot_tn(z_mid, grad_y))
    g_at_qkv = dot_tn(jnp.concatenate(dmids, axis=1), normed_f32)
    parts = [g_at_qkv[:rank], g_at_qkv[rank:2 * rank], g_at_qkv[2 * rank:], g_at_o, bs[0], g_b_o, bs[1], bs[2]]
    packed = all_reduce_rows(jnp.concatenate(parts, axis=1), 2)
    sums = []
    at = 0
    for part in parts:
        sums.append(packed[:, at:at + part.shape[1]])
        at += part.shape[1]
    at_q, at_k, at_v, at_o, gb_q, gb_o, gb_k, gb_v = sums
    g_a_gate, g_b_gate, g_a_up, g_b_up, g_a_down_t, g_b_down = mlp_grads
    return hidden_next, (at_q.T, gb_q, at_k.T, gb_k, at_v.T, gb_v, at_o.T, gb_o,
                         g_a_gate, g_b_gate, g_a_up, g_b_up, g_a_down_t.T, g_b_down)


def solution(mesh):
    tok_spec = P(AXIS)
    row_spec = P(None, AXIS)
    rep_spec = P()
    in_specs = (tok_spec, tok_spec, rep_spec, rep_spec) + (row_spec,) * 7 + (rep_spec,) * 14
    out_specs = (tok_spec,) + (rep_spec,) * 14

    def per_device(hidden_in, grad_out, gain_attn, gain_mlp, *weights):
        n_seq, seq_len, model_dim = hidden_in.shape
        base = tuple(w[0] for w in weights[:7])
        lora = tuple(w[0] for w in weights[7:])
        hidden_next, grads = layer_step(hidden_in.reshape(-1, model_dim), grad_out.reshape(-1, model_dim), seq_len,
                                        gain_attn[0], gain_mlp[0], base, lora)
        return (hidden_next.reshape(hidden_in.shape),) + tuple(g[None] for g in grads)

    return jax.shard_map(per_device, mesh=mesh, in_specs=in_specs, out_specs=out_specs, check_vma=False)
```

```python
import functools

import jax
import jax.numpy as jnp
from jax import lax
from jax.experimental import pallas as pl
from jax.experimental.pallas import tpu as pltpu
from jax.sharding import PartitionSpec as P

LORA_SCALE = 2.0
NORM_EPS = 1e-5
ROPE_BASE = 10000.0
AXIS = 'fsdp'
F32 = jnp.float32
BF16 = jnp.bfloat16
FF_CHUNK = 256
DOWN_COLS = 512
N_SPANS = 4


def rms_norm(hidden, gain_vec):
    hid_f32 = hidden.astype(F32)
    inv_rms = lax.rsqrt(jnp.mean(hid_f32 * hid_f32, axis=-1, keepdims=True) + NORM_EPS)
    return (hid_f32 * inv_rms * gain_vec.astype(F32)).astype(BF16)


def apply_rope(rot_in):
    seq_len, head_dim = rot_in.shape[1], rot_in.shape[3]
    half_dim = head_dim // 2
    inv_freq = ROPE_BASE ** (-jnp.arange(half_dim, dtype=F32) * 2.0 / head_dim)
    angles = jnp.arange(seq_len, dtype=F32)[:, None] * inv_freq[None, :]
    cos_t = jnp.cos(angles)[:, None, :]
    sin_t = jnp.sin(angles)[:, None, :]
    first_half = rot_in[..., :half_dim]
    second_half = rot_in[..., half_dim:]
    return jnp.concatenate([first_half * cos_t - second_half * sin_t, second_half * cos_t + first_half * sin_t], axis=-1)


def attn_core(q_proj, k_proj, v_proj):
    n_seq, seq_len, n_heads, head_dim = q_proj.shape
    kv_heads = k_proj.shape[2]
    q_rot = apply_rope(q_proj).astype(BF16).reshape(n_seq, seq_len, kv_heads, n_heads // kv_heads, head_dim)
    k_rot = apply_rope(k_proj).astype(BF16)
    scores = jnp.einsum('bqkgd,bskd->bkgqs', q_rot, k_rot, preferred_element_type=F32) * (head_dim ** -0.5)
    causal = jnp.arange(seq_len)[:, None] >= jnp.arange(seq_len)[None, :]
    attn_probs = jax.nn.softmax(jnp.where(causal, scores, -1e30), axis=-1).astype(BF16)
    attn_out = jnp.einsum('bkgqs,bskd->bqkgd', attn_probs, v_proj, preferred_element_type=F32)
    return attn_out.astype(BF16).reshape(n_seq * seq_len, n_heads * head_dim)


def dot_nn(a, b):
    return lax.dot_general(a, b, (((1,), (0,)), ((), ())), preferred_element_type=F32)


def dot_nt(a, b):
    return lax.dot_general(a, b, (((1,), (1,)), ((), ())), preferred_element_type=F32)


def dot_tn(a, b):
    return lax.dot_general(a, b, (((0,), (0,)), ((), ())), preferred_element_type=F32)


def coords():
    me = lax.axis_index(AXIS)
    core = lax.rem(me, 2)
    x = lax.rem(me // 2, 2)
    y = lax.rem(me // 4, 2)
    z = me // 8
    return me, z, y, x, core


def peers(me, z, y, x, core):
    z_peers = [me + 8 * (lax.rem(z + k, 4) - z) for k in (1, 2, 3)]
    return z_peers, me + 4 * (1 - 2 * y), me + 2 * (1 - 2 * x), me + 1 - 2 * core


def entry_barrier(devices):
    barrier = pltpu.get_barrier_semaphore()
    for dev in devices:
        pl.semaphore_signal(barrier, inc=1, device_id=(dev,), device_id_type=pl.DeviceIdType.MESH)
    pl.semaphore_wait(barrier, len(devices))


def remote(src, dst, send_sem, recv_sem, dev):
    return pltpu.make_async_remote_copy(src_ref=src, dst_ref=dst, send_sem=send_sem, recv_sem=recv_sem,
                                        device_id=(dev,), device_id_type=pl.DeviceIdType.MESH)


N_COPIES = 14


def gather_phase(src, out, phase, row, n_rows, send, recv):
    me, z, y, x, core = coords()
    z_peers, y_peer, x_peer, partner = peers(me, z, y, x, core)
    tiles = n_rows // 8
    n_c = tiles // 8
    n_a = (tiles - n_c + 1) // 2
    n_b = tiles - n_c - n_a
    a_rows = pl.ds(row, 8 * n_a)
    b_rows = pl.ds(row + 8 * n_a, 8 * n_b)
    ab_rows = pl.ds(row, 8 * (n_a + n_b))
    c_rows = pl.ds(row + 8 * (n_a + n_b), 8 * n_c)
    if phase == 0:
        items = [(src.at[ab_rows], out.at[z, y, x, core, ab_rows], dev) for dev in z_peers]
        if n_c:
            items.append((src.at[c_rows], out.at[z, y, x, core, c_rows], x_peer))
    elif phase == 1:
        items = [(out.at[:, y, x, core, a_rows], y_peer), (out.at[:, y, x, core, b_rows], x_peer)]
        if n_c:
            items.append((out.at[z, y, :, core, c_rows], y_peer))
    elif phase == 2:
        items = [(out.at[:, :, x, core, a_rows], x_peer), (out.at[:, y, :, core, b_rows], y_peer)]
        if n_c:
            items += [(out.at[z, :, :, core, c_rows], dev) for dev in z_peers]
    else:
        items = [(out.at[:, :, :, core, pl.ds(row, n_rows)], partner)]
    base = (0, 4, 7, 12)[phase]
    copies = []
    for k, item in enumerate(items):
        s_ref, d_ref, dev = item if len(item) == 3 else (item[0],) + item
        copies.append(remote(s_ref, d_ref, send.at[base + k], recv.at[base + k], dev))
    return copies


def gather_rows_kernel(n_arr, *refs):
    srcs, outs = refs[:n_arr], refs[n_arr:2 * n_arr]
    send, recv, own_sem = refs[2 * n_arr:]
    me, z, y, x, core = coords()
    z_peers, y_peer, x_peer, partner = peers(me, z, y, x, core)
    entry_barrier(z_peers + [y_peer, x_peer, partner])
    def own_copy(i):
        return pltpu.make_async_copy(srcs[i], outs[i].at[z, y, x, core], own_sem.at[i])

    for i in range(n_arr):
        own_copy(i).start()
    for i in range(n_arr):
        own_copy(i).wait()

    spans = []
    for src in srcs:
        rows = src.shape[0]
        step = -(-rows // (8 * N_SPANS)) * 8
        spans.append([(at, min(step, rows - at)) for at in range(0, rows, step)])
    n_ticks = max(len(s) for s in spans)

    def tick_copies(tick, i):
        live = []
        for phase in (2, 1, 0, 3):
            if 0 <= tick - phase < len(spans[i]):
                row, n_rows = spans[i][tick - phase]
                live += gather_phase(srcs[i], outs[i], phase, row, n_rows, send.at[tick % 2, i], recv.at[tick % 2, i])
        return live

    for tick in range(n_ticks + 4):
        for i in range(n_arr):
            for copy in tick_copies(tick - 1, i):
                copy.wait()
            for copy in tick_copies(tick, i):
                copy.start()


def gather_rows(mats, collective_id):
    n_arr = len(mats)
    outs = pl.pallas_call(
        functools.partial(gather_rows_kernel, n_arr),
        out_shape=[jax.ShapeDtypeStruct((4, 2, 2, 2) + m.shape, m.dtype) for m in mats],
        in_specs=[pl.BlockSpec(memory_space=pltpu.VMEM)] * n_arr,
        out_specs=[pl.BlockSpec(memory_space=pl.ANY)] * n_arr,
        scratch_shapes=[
            pltpu.SemaphoreType.DMA((2, n_arr, N_COPIES)),
            pltpu.SemaphoreType.DMA((2, n_arr, N_COPIES)),
            pltpu.SemaphoreType.DMA((n_arr,)),
        ],
        compiler_params=pltpu.CompilerParams(collective_id=collective_id, has_side_effects=True),
        name='gather_rows',
    )(*mats)
    return [o.reshape(32 * m.shape[0], m.shape[1]) for o, m in zip(outs, mats)]


def all_reduce_kernel(x_in, out, acc, r_core, r2a, r2b, r3a, r3b, r4, send, recv):
    me, z, y, x, core = coords()
    z_peers, y_peer, x_peer, partner = peers(me, z, y, x, core)
    entry_barrier(z_peers + [y_peer, x_peer, partner])
    block = x_in.shape[3] // 4
    wide = r3a.shape[2]

    def cols(yy, xx):
        return pl.ds(pl.multiple_of((yy * 2 + xx) * block, 128), block)

    def cols_a(yy, xx):
        return pl.ds(pl.multiple_of((yy * 2 + xx) * block, 128), wide)

    def cols_b(yy, xx):
        return pl.ds(pl.multiple_of((yy * 2 + xx) * block + wide, 128), block - wide)

    used = [0]

    def exchange(items):
        copies = []
        for src, dst, dev in items:
            copies.append(remote(src, dst, send.at[used[0]], recv.at[used[0]], dev))
            used[0] += 1
        for copy in copies:
            copy.start()
        for copy in copies:
            copy.wait()

    exchange([(x_in.at[1 - core], r_core, partner)])
    acc[...] = x_in[core] + r_core[...]
    exchange([(acc.at[:, :, cols_a(i, 1 - x)], r2a.at[i], x_peer) for i in range(2)]
             + [(acc.at[:, :, cols_b(1 - y, i)], r2b.at[i], y_peer) for i in range(2)])
    for i in range(2):
        acc[:, :, cols_a(i, x)] += r2a[i]
        acc[:, :, cols_b(y, i)] += r2b[i]
    exchange([(acc.at[:, :, cols_a(1 - y, x)], r3a, y_peer), (acc.at[:, :, cols_b(y, 1 - x)], r3b, x_peer)])
    acc[:, :, cols_a(y, x)] += r3a[...]
    acc[:, :, cols_b(y, x)] += r3b[...]
    here = cols(y, x)
    exchange([(acc.at[lax.rem(z + k + 1, 4), :, here], r4.at[k], z_peers[k]) for k in range(3)])
    out[core, z, :, here] = acc[z, :, here] + (r4[0] + r4[1] + r4[2])
    exchange([(out.at[core, z, :, here], out.at[core, z, :, here], dev) for dev in z_peers])

    def same(at, dev):
        ref = out.at[core, :, :, at]
        return ref, ref, dev

    exchange([same(cols_a(y, x), y_peer), same(cols_b(y, x), x_peer)])
    exchange([same(cols_a(i, x), x_peer) for i in range(2)] + [same(cols_b(y, i), y_peer) for i in range(2)])
    exchange([(out.at[core], out.at[core], partner)])


def all_reduce_rows(x, collective_id):
    n = x.shape[1]
    block = n // 4
    wide = (block // 256 + (block // 128) % 2) * 128
    vmem = pl.BlockSpec(memory_space=pltpu.VMEM)
    out = pl.pallas_call(
        all_reduce_kernel,
        out_shape=jax.ShapeDtypeStruct((2, 4, 8, n), F32),
        in_specs=[vmem],
        out_specs=vmem,
        scratch_shapes=[
            pltpu.VMEM((4, 8, n), F32),
            pltpu.VMEM((4, 8, n), F32),
            pltpu.VMEM((2, 4, 8, wide), F32),
            pltpu.VMEM((2, 4, 8, block - wide), F32),
            pltpu.VMEM((4, 8, wide), F32),
            pltpu.VMEM((4, 8, block - wide), F32),
            pltpu.VMEM((3, 8, block), F32),
            pltpu.SemaphoreType.DMA((20,)),
            pltpu.SemaphoreType.DMA((20,)),
        ],
        compiler_params=pltpu.CompilerParams(collective_id=collective_id, has_side_effects=True),
        name='all_reduce_rows',
    )(x.reshape(2, 4, 8, n))
    return out.reshape(64, n)


def mlp_kernel(u, dout, zg, zu, dmd, zg_t, zu_t, dmd_t, w_loc, b_gate, b_up, a_down_t, w_down_a, w_down_b,
               down_out, back_out, z_down, dm_gate, dm_up, gb_gate, gb_up, ga_down_t, full,
               w_gu, w_dn, send, recv, own_sem, load_sem):
    n_chunks = w_loc.shape[0]
    width = w_loc.shape[3]
    rows = 32 * w_loc.shape[2]
    me, z, y, x, core = coords()
    z_peers, y_peer, x_peer, partner = peers(me, z, y, x, core)
    entry_barrier(z_peers + [y_peer, x_peer, partner])
    own = pltpu.make_async_copy(w_loc, full.at[:, :, z, y, x, core], own_sem)
    own.start()
    own.wait()

    def phase_copies(chunk, phase, par, part):
        return gather_phase(w_loc.at[chunk, part], full.at[chunk, part], phase, 0, w_loc.shape[2],
                            send.at[par, part], recv.at[par, part])

    down_out[...] = jnp.zeros_like(down_out)
    back_out[...] = jnp.zeros_like(back_out)
    z_down[...] = jnp.zeros_like(z_down)
    dm_gate[...] = jnp.zeros_like(dm_gate)
    dm_up[...] = jnp.zeros_like(dm_up)

    def loads(chunk):
        at = pl.multiple_of(chunk * width, width)
        return (pltpu.make_async_copy(full.at[chunk, 0], w_gu.at[0], load_sem.at[0]),
                pltpu.make_async_copy(full.at[chunk, 1], w_gu.at[1], load_sem.at[1]),
                pltpu.make_async_copy(w_down_a.at[pl.ds(at, width), :], w_dn.at[:, pl.ds(0, DOWN_COLS)], load_sem.at[2]),
                pltpu.make_async_copy(w_down_b.at[pl.ds(at, width), :], w_dn.at[:, pl.ds(DOWN_COLS, w_dn.shape[1] - DOWN_COLS)], load_sem.at[3]))

    def compute(chunk):
        at = pl.multiple_of(chunk * width, width)
        cols = pl.ds(at, width)
        load_g, load_u, load_a, load_b = loads(chunk)
        load_g.start()
        load_u.start()
        load_a.start()
        load_b.start()
        bg, bu, ad = b_gate[:, cols], b_up[:, cols], a_down_t[:, cols]
        load_g.wait()
        wg = w_gu[0].reshape(rows, width)
        gate = dot_nn(u[...], wg) + LORA_SCALE * dot_nn(zg[...], bg)
        load_u.wait()
        wu = w_gu[1].reshape(rows, width)
        up = dot_nn(u[...], wu) + LORA_SCALE * dot_nn(zu[...], bu)
        sig = jax.nn.sigmoid(gate)
        silu = gate * sig
        act = (silu * up).astype(BF16)
        load_a.wait()
        load_b.wait()
        grad_act = (dot_nt(dout[...], w_dn[...]) + dot_nn(dmd[...], ad)).astype(BF16).astype(F32)
        d_up = grad_act * silu
        d_gate = grad_act * up * (sig + silu * (1.0 - sig))
        down_out[...] += dot_nn(act, w_dn[...])
        z_down[...] += dot_nt(act.astype(F32), ad)
        ga_down_t[:, cols] = dot_nn(dmd_t[...], act.astype(F32))
        gb_gate[:, cols] = LORA_SCALE * dot_nn(zg_t[...], d_gate)
        gb_up[:, cols] = LORA_SCALE * dot_nn(zu_t[...], d_up)
        dm_gate[...] += LORA_SCALE * dot_nt(d_gate, bg)
        dm_up[...] += LORA_SCALE * dot_nt(d_up, bu)
        back_out[...] += dot_nt(d_gate.astype(BF16), wg) + dot_nt(d_up.astype(BF16), wu)

    def each_copy(tick, part, act):
        par = lax.rem(tick + 2, 2)
        for phase in (2, 1, 0, 3):
            chunk = tick - phase

            @pl.when((chunk >= 0) & (chunk < n_chunks))
            def _(chunk=chunk, phase=phase):
                for copy in phase_copies(chunk, phase, par, part):
                    act(copy)

    def tick_body(tick, carry):
        for part in range(2):
            each_copy(tick - 1, part, lambda copy: copy.wait())
            each_copy(tick, part, lambda copy: copy.start())

        @pl.when(tick >= 4)
        def _():
            compute(tick - 4)
        return carry

    lax.fori_loop(0, n_chunks + 4, tick_body, 0)


def fused_mlp(u, dout, zg, zu, dmd, w_gate, w_up, b_gate, b_up, a_down_t, w_down_a, w_down_b, collective_id):
    tokens, model_dim = u.shape
    shard, ff = w_gate.shape
    rank = zg.shape[1]
    n_chunks = ff // FF_CHUNK
    w_loc = jnp.stack([w_gate, w_up]).reshape(2, shard, n_chunks, FF_CHUNK).transpose(2, 0, 1, 3)
    vmem = pl.BlockSpec(memory_space=pltpu.VMEM)
    hbm = pl.BlockSpec(memory_space=pl.ANY)
    f32 = lambda *s: jax.ShapeDtypeStruct(s, F32)
    outs = pl.pallas_call(
        mlp_kernel,
        out_shape=[f32(tokens, model_dim), f32(tokens, model_dim), f32(tokens, rank), f32(tokens, rank), f32(tokens, rank),
                   f32(rank, ff), f32(rank, ff), f32(rank, ff),
                   jax.ShapeDtypeStruct((n_chunks, 2, 4, 2, 2, 2, shard, FF_CHUNK), BF16)],
        in_specs=[vmem] * 12 + [hbm] * 2,
        out_specs=[vmem] * 8 + [hbm],
        scratch_shapes=[
            pltpu.VMEM((2, 4, 2, 2, 2, shard, FF_CHUNK), BF16),
            pltpu.VMEM((FF_CHUNK, model_dim), BF16),
            pltpu.SemaphoreType.DMA((2, 2, N_COPIES)),
            pltpu.SemaphoreType.DMA((2, 2, N_COPIES)),
            pltpu.SemaphoreType.DMA,
            pltpu.SemaphoreType.DMA((4,)),
        ],
        compiler_params=pltpu.CompilerParams(collective_id=collective_id, has_side_effects=True, vmem_limit_bytes=60 * 2 ** 20),
        cost_estimate=pl.CostEstimate(flops=12 * tokens * model_dim * ff, bytes_accessed=6 * model_dim * ff, transcendentals=0),
        name='fused_mlp',
    )(u, dout, zg, zu, dmd, zg.T, zu.T, dmd.T, w_loc, b_gate, b_up, a_down_t, w_down_a, w_down_b)
    return outs[:8]


def layer_step(hidden, grad_next, seq_len, gain_attn, gain_mlp, base_shards, lora):
    w_q, w_k, w_v, w_o, w_gate, w_up, w_down = base_shards
    a_q, b_q, a_k, b_k, a_v, b_v, a_o, b_o, a_gate, b_gate, a_up, b_up, a_down, b_down = lora
    tokens, model_dim = hidden.shape
    n_seq = tokens // seq_len
    shard = w_q.shape[0]
    n_heads, head_dim = w_q.shape[1:]
    kv_heads = w_k.shape[1]
    q_dim, k_dim = n_heads * head_dim, kv_heads * head_dim
    rank = a_q.shape[1]
    w_qkv_loc = jnp.concatenate([w_q.reshape(shard, q_dim), w_k.reshape(shard, k_dim), w_v.reshape(shard, k_dim)], axis=1)
    w_half = w_qkv_loc.shape[1] // 2
    w_qkv_a, w_qkv_b, w_down_a = gather_rows([w_qkv_loc[:, :w_half], w_qkv_loc[:, w_half:], w_down[:, :DOWN_COLS]], 0)
    w_o_full = lax.all_gather(w_o, AXIS, axis=0, tiled=True)
    w_down_b = lax.all_gather(w_down[:, DOWN_COLS:], AXIS, axis=0, tiled=True)

    normed, norm_attn_pull = jax.vjp(lambda h: rms_norm(h, gain_attn), hidden)
    a_qkv = jnp.concatenate([a_q, a_k, a_v], axis=1)
    z_qkv = jnp.dot(normed, a_qkv, preferred_element_type=F32)
    z_q, z_k, z_v = z_qkv[:, :rank], z_qkv[:, rank:2 * rank], z_qkv[:, 2 * rank:]
    qkv = jnp.concatenate([dot_nn(normed, w_qkv_a), dot_nn(normed, w_qkv_b)], axis=1)
    q_flat = qkv[:, :q_dim] + LORA_SCALE * dot_nn(z_q, b_q)
    k_flat = qkv[:, q_dim:q_dim + k_dim] + LORA_SCALE * dot_nn(z_k, b_k)
    v_flat = qkv[:, q_dim + k_dim:] + LORA_SCALE * dot_nn(z_v, b_v)
    q_proj = q_flat.reshape(n_seq, seq_len, n_heads, head_dim)
    k_proj = k_flat.reshape(n_seq, seq_len, kv_heads, head_dim)
    v_proj = v_flat.astype(BF16).reshape(n_seq, seq_len, kv_heads, head_dim)
    attn_out, attn_pull = jax.vjp(attn_core, q_proj, k_proj, v_proj)
    z_o = jnp.dot(attn_out, a_o, preferred_element_type=F32)
    o_full = dot_nn(attn_out, w_o_full) + LORA_SCALE * dot_nn(z_o, b_o)
    h_mid = (hidden.astype(F32) + o_full).astype(BF16)
    normed_mlp, norm_mlp_pull = jax.vjp(lambda h: rms_norm(h, gain_mlp), h_mid)

    z_gu = jnp.dot(normed_mlp, jnp.concatenate([a_gate, a_up], axis=1), preferred_element_type=F32)
    z_gate, z_up = z_gu[:, :rank], z_gu[:, rank:]
    dmid_down = LORA_SCALE * dot_nt(grad_next.astype(F32), b_down)
    down_out, back, z_down, dmid_gate, dmid_up, g_b_gate, g_b_up, g_a_down_t = fused_mlp(
        normed_mlp, grad_next, z_gate, z_up, dmid_down, w_gate, w_up, b_gate, b_up, a_down.T, w_down_a, w_down_b, 1)
    hidden_next = (h_mid.astype(F32) + down_out + LORA_SCALE * dot_nn(z_down, b_down)).astype(BF16)
    g_b_down = LORA_SCALE * dot_tn(z_down, grad_next.astype(F32))
    g_a_gate = dot_tn(normed_mlp.astype(F32), dmid_gate)
    g_a_up = dot_tn(normed_mlp.astype(F32), dmid_up)
    mlp_grads = lax.psum((g_a_gate, g_b_gate, g_a_up, g_b_up, g_a_down_t, g_b_down), AXIS)
    back = back + dot_nt(dmid_gate, a_gate) + dot_nt(dmid_up, a_up)
    grad_norm_mlp = norm_mlp_pull(back.astype(BF16))[0]
    grad_mid = (grad_next.astype(F32) + grad_norm_mlp.astype(F32)).astype(BF16)

    grad_mid_f32 = grad_mid.astype(F32)
    dmid_o = LORA_SCALE * dot_nt(grad_mid_f32, b_o)
    grad_attn = dot_nt(grad_mid, w_o_full) + dot_nt(dmid_o, a_o)
    g_at_o = dot_tn(dmid_o, attn_out.astype(F32))
    g_b_o = LORA_SCALE * dot_tn(z_o, grad_mid_f32)
    grad_q, grad_k, grad_v = attn_pull(grad_attn.astype(BF16))
    grad_q = grad_q.reshape(tokens, -1).astype(F32)
    grad_k = grad_k.reshape(tokens, -1).astype(F32)
    grad_v = grad_v.reshape(tokens, -1).astype(F32)
    normed_f32 = normed.astype(F32)
    dmids = []
    bs = []
    for z_mid, grad_y, b_mat in ((z_q, grad_q, b_q), (z_k, grad_k, b_k), (z_v, grad_v, b_v)):
        dmids.append(LORA_SCALE * dot_nt(grad_y, b_mat))
        bs.append(LORA_SCALE * dot_tn(z_mid, grad_y))
    g_at_qkv = dot_tn(jnp.concatenate(dmids, axis=1), normed_f32)
    parts = [g_at_qkv[:rank], g_at_qkv[rank:2 * rank], g_at_qkv[2 * rank:], g_at_o, bs[0], g_b_o, bs[1], bs[2]]
    parts, hidden_next = lax.optimization_barrier((parts, hidden_next))
    packed = all_reduce_rows(jnp.concatenate(parts, axis=1), 2)
    sums = []
    at = 0
    for part in parts:
        sums.append(packed[:, at:at + part.shape[1]])
        at += part.shape[1]
    at_q, at_k, at_v, at_o, gb_q, gb_o, gb_k, gb_v = sums
    g_a_gate, g_b_gate, g_a_up, g_b_up, g_a_down_t, g_b_down = mlp_grads
    return hidden_next, (at_q.T, gb_q, at_k.T, gb_k, at_v.T, gb_v, at_o.T, gb_o,
                         g_a_gate, g_b_gate, g_a_up, g_b_up, g_a_down_t.T, g_b_down)


def solution(mesh):
    tok_spec = P(AXIS)
    row_spec = P(None, AXIS)
    rep_spec = P()
    in_specs = (tok_spec, tok_spec, rep_spec, rep_spec) + (row_spec,) * 7 + (rep_spec,) * 14
    out_specs = (tok_spec,) + (rep_spec,) * 14

    def per_device(hidden_in, grad_out, gain_attn, gain_mlp, *weights):
        n_seq, seq_len, model_dim = hidden_in.shape
        base = tuple(w[0] for w in weights[:7])
        lora = tuple(w[0] for w in weights[7:])
        hidden_next, grads = layer_step(hidden_in.reshape(-1, model_dim), grad_out.reshape(-1, model_dim), seq_len,
                                        gain_attn[0], gain_mlp[0], base, lora)
        return (hidden_next.reshape(hidden_in.shape),) + tuple(g[None] for g in grads)

    return jax.shard_map(per_device, mesh=mesh, in_specs=in_specs, out_specs=out_specs, check_vma=False)
```
